16 devices in a mesh: ez: 2 (over z), ey: 2 (over y), ex: 4 (over x, core).
Axes of the slice: x: 2, y: 2, z: 2, core: 2. Of those that a mesh axis runs over, the one named last changes fastest.
Arguments:
- tokens_in: bfloat16 [2, 4096, 1024], P(None, ('ez', 'ey', 'ex'))
- expert_ids: int32 [2, 2, 4096, 8], P(None, None, ('ez', 'ey', 'ex'))
- gate_vals: float32 [2, 2, 4096, 8], P(None, None, ('ez', 'ey', 'ex'))
- w_up1: bfloat16 [2, 32, 1024, 512], P(None, ('ez', 'ey', 'ex'))
- w_up3: bfloat16 [2, 32, 1024, 512], P(None, ('ez', 'ey', 'ex'))
- w_down: bfloat16 [2, 32, 512, 1024], P(None, ('ez', 'ey', 'ex'))
Outputs:
- output: bfloat16 [2, 4096, 1024], P(None, ('ez', 'ey', 'ex'))
All inputs are finite; a program needn't handle non-finite values.
Results may differ from the reference program's by a relative error of at most 0.0106397.
Values are sent between devices in bfloat16 or wider.
A program may use at most 1 GiB of HBM per device.

```python
import jax
import jax.numpy as jnp
import numpy as np
from jax import lax

HIDDEN = 1024
FFN_DIM = 512
EXPERTS = 32
TOP_K = 8
TOK_MB = 256
DEVICES = 16
LAYERS = 2
MICRO_BATCHES = 2
CAPACITY = 2 * ((TOK_MB * TOP_K + EXPERTS - 1) // EXPERTS)
ROWS_MAX = DEVICES * CAPACITY
ROUTE_SCALE = 2.5


def rank_table():
    hot_count = EXPERTS // 16 + 1
    rest_total = TOK_MB * TOP_K - hot_count * CAPACITY
    cold_count = EXPERTS - hot_count
    base_share = rest_total // cold_count
    extra_count = rest_total % cold_count
    counts = [CAPACITY] * hot_count + [base_share + 1] * extra_count + [base_share] * (cold_count - extra_count)
    return np.repeat(np.arange(EXPERTS), counts).reshape(TOP_K, TOK_MB).T.astype(np.int32)


def route_block(key):
    key_perm, key_tok, key_roll = jax.random.split(key, 3)
    expert_perm = jax.random.permutation(key_perm, EXPERTS)
    chosen = expert_perm[jnp.asarray(rank_table())]
    chosen = chosen[jax.random.permutation(key_tok, TOK_MB)]
    roll_shift = jax.random.randint(key_roll, (TOK_MB, 1), 0, TOP_K)
    slot_order = (jnp.arange(TOP_K)[None, :] + roll_shift) % TOP_K
    return jnp.take_along_axis(chosen, slot_order, axis=1).astype(jnp.int32)


def setup_inputs(seed: int = 0) -> dict:
    key = jax.random.key(seed)
    key_x, key_ids, key_gate, key_up1, key_up3, key_down = jax.random.split(key, 6)
    n_tokens = DEVICES * TOK_MB
    tokens_in = jax.random.normal(key_x, (MICRO_BATCHES, n_tokens, HIDDEN), jnp.float32).astype(jnp.bfloat16)
    block_keys = jax.random.split(key_ids, LAYERS * MICRO_BATCHES * DEVICES)
    expert_ids = jax.vmap(route_block)(block_keys).reshape(LAYERS, MICRO_BATCHES, n_tokens, TOP_K)
    raw_gates = jax.random.uniform(key_gate, (LAYERS, MICRO_BATCHES, n_tokens, TOP_K), jnp.float32, 0.25, 1.75)
    gate_vals = raw_gates / jnp.sum(raw_gates, axis=-1, keepdims=True)
    up_shape = (LAYERS, EXPERTS, HIDDEN, FFN_DIM)
    w_up1 = (jax.random.normal(key_up1, up_shape, jnp.float32) * HIDDEN ** -0.5).astype(jnp.bfloat16)
    w_up3 = (jax.random.normal(key_up3, up_shape, jnp.float32) * HIDDEN ** -0.5).astype(jnp.bfloat16)
    w_down = (jax.random.normal(key_down, (LAYERS, EXPERTS, FFN_DIM, HIDDEN), jnp.float32) * FFN_DIM ** -0.5).astype(jnp.bfloat16)
    return {"tokens_in": tokens_in, "expert_ids": expert_ids, "gate_vals": gate_vals, "w_up1": w_up1, "w_up3": w_up3, "w_down": w_down}


def moe_layer(tokens, ids_mb, gates_mb, mat_up1, mat_up3, mat_down):
    n_assign = tokens.shape[0] * TOP_K
    flat_ids = ids_mb.reshape(n_assign)
    sort_order = jnp.argsort(flat_ids, stable=True)
    counts = jnp.bincount(flat_ids, length=EXPERTS)
    starts = jnp.cumsum(counts) - counts
    row_pos = jnp.arange(ROWS_MAX)

    def one_expert(operands):
        first_row, row_count, mat_a, mat_b, mat_c = operands
        picked = sort_order[jnp.minimum(first_row + row_pos, n_assign - 1)]
        expert_rows = tokens[picked // TOP_K]
        gate_in = jnp.dot(expert_rows, mat_a, preferred_element_type=jnp.float32)
        lin_in = jnp.dot(expert_rows, mat_b, preferred_element_type=jnp.float32)
        hidden = (jax.nn.silu(gate_in) * lin_in).astype(jnp.bfloat16)
        expert_out = jnp.dot(hidden, mat_c, preferred_element_type=jnp.float32).astype(jnp.bfloat16)
        return expert_out, jnp.where(row_pos < row_count, picked, n_assign)

    all_out, targets = lax.map(one_expert, (starts, counts, mat_up1, mat_up3, mat_down))
    per_assign = jnp.zeros((n_assign + 1, HIDDEN), jnp.bfloat16).at[targets.reshape(-1)].set(all_out.reshape(-1, HIDDEN))
    per_assign = per_assign[:n_assign].reshape(tokens.shape[0], TOP_K, HIDDEN)
    moe_sum = jnp.einsum("tj,tjh->th", gates_mb.astype(jnp.float32), per_assign.astype(jnp.float32))
    return (tokens.astype(jnp.float32) + ROUTE_SCALE * moe_sum).astype(jnp.bfloat16)


def reference(tokens_in, expert_ids, gate_vals, w_up1, w_up3, w_down):
    def layer_step(layer_in, layer_args):
        ids_layer, gates_layer, mat_up1, mat_up3, mat_down = layer_args

        def one_batch(batch_args):
            batch_tok, ids_mb, gates_mb = batch_args
            return moe_layer(batch_tok, ids_mb, gates_mb, mat_up1, mat_up3, mat_down)

        return lax.map(one_batch, (layer_in, ids_layer, gates_layer)), None

    tokens_out, _ = lax.scan(layer_step, tokens_in, (expert_ids, gate_vals, w_up1, w_up3, w_down))
    return tokens_out
```

```python
import jax
import jax.numpy as jnp
from jax import lax
from jax.sharding import PartitionSpec as P

ROUTE_SCALE = 2.5
MESH_AXES = ("ez", "ey", "ex")


def solution(mesh):
    n_dev = mesh.shape["ez"] * mesh.shape["ey"] * mesh.shape["ex"]
    tok_spec = P(None, MESH_AXES, None)
    route_spec = P(None, None, MESH_AXES, None)
    weight_spec = P(None, MESH_AXES, None, None)

    def device_body(tokens_in, expert_ids, gate_vals, w_up1, w_up3, w_down):
        n_layers, n_micro, tok_mb, top_k = expert_ids.shape
        exp_dev = w_up1.shape[1]
        experts = exp_dev * n_dev
        hot = expert_ids[..., None] == jnp.arange(experts)
        table = jnp.sum(jnp.where(hot, gate_vals[..., None], 0.0), axis=-2)
        table = table.reshape(n_layers, n_micro, tok_mb, n_dev, exp_dev)
        table = lax.all_to_all(table, MESH_AXES, 3, 2, tiled=True)
        table = table.reshape(n_layers, n_micro, n_dev * tok_mb, exp_dev)
        batches = [tokens_in[mb_idx] for mb_idx in range(n_micro)]
        for layer_idx in range(n_layers):
            for mb_idx in range(n_micro):
                tokens = batches[mb_idx]
                everyone = lax.all_gather(tokens, MESH_AXES, axis=0, tiled=True)
                total = jnp.zeros(everyone.shape, jnp.float32)
                for e in range(exp_dev):
                    a = jnp.dot(everyone, w_up1[layer_idx, e], preferred_element_type=jnp.float32)
                    b = jnp.dot(everyone, w_up3[layer_idx, e], preferred_element_type=jnp.float32)
                    h = (jax.nn.silu(a) * b).astype(jnp.bfloat16)
                    o = jnp.dot(h, w_down[layer_idx, e], preferred_element_type=jnp.float32).astype(jnp.bfloat16)
                    g = table[layer_idx, mb_idx, :, e][:, None]
                    total = total + jnp.where(g > 0.0, g * o.astype(jnp.float32), 0.0)
                moe_sum = lax.psum_scatter(total, MESH_AXES, scatter_dimension=0, tiled=True)
                batches[mb_idx] = (tokens.astype(jnp.float32) + ROUTE_SCALE * moe_sum).astype(jnp.bfloat16)
        return jnp.stack(batches)

    return jax.shard_map(device_body, mesh=mesh, in_specs=(tok_spec, route_spec, route_spec, weight_spec, weight_spec, weight_spec), out_specs=tok_spec, check_vma=False)
```

```python
import functools

import jax
import jax.numpy as jnp
from jax import lax
from jax.experimental import pallas as pl
from jax.experimental.pallas import tpu as pltpu
from jax.sharding import PartitionSpec as P

ROUTE_SCALE = 2.5
MESH_AXES = ("ez", "ey", "ex")
MESH = pl.DeviceIdType.MESH
BF16, F32 = jnp.bfloat16, jnp.float32

TOK, HID, FFN = 256, 1024, 512
PARTS = (96, 80, 80)
OFFS = (0, 96, 176)
HALF = 4 * TOK
CHUNK = 256
CHUNKS = 8 * TOK // CHUNK
STAGES = 4

AXES_OF = tuple(((k + 2) % 3, (k + 1) % 3, k) for k in range(3))
GATHER = ((0, 1, 2), (0, 2, 1), (0, 4, 0), (1, 3, 1), (1, 5, 0), (2, 6, 0), (3, 7, 0))


def base(place, k):
    return (place // 4) * HALF + 4 * OFFS[k] + (place % 4) * PARTS[k]


def bits_of(place, k):
    bits = [0, 0, 0]
    for weight, axis in zip((4, 2, 1), AXES_OF[k]):
        bits[axis] = 1 if place & weight else 0
    return bits


def moe_kernel(tok, ids, gts, w1h, w3h, w2h, out, xbuf, pbuf, ra, rb, rc, w1, w3, w2, tt, gr, gbuf, fin,
               ag_s, ag_r, rs_s, rs_r, wl_s, wr_s, wr_r, g_s, g_r, t_s, o_s, credit, wfree):
    z, y, ex = (lax.axis_index(name) for name in MESH_AXES)
    x, core = ex // 2, ex % 2

    def dev(bx, by, bz):
        xx = 1 - x if bx else x
        return (1 - z if bz else z, 1 - y if by else y, xx * 2 + core)

    nbr = (dev(1, 0, 0), dev(0, 1, 0), dev(0, 0, 1))
    sib = (z, y, x * 2 + 1 - core)

    def remote(src, dst, ss, rs, to):
        return pltpu.make_async_remote_copy(src_ref=src, dst_ref=dst, send_sem=ss, recv_sem=rs, device_id=to, device_id_type=MESH)

    def ag(s, k, j):
        src, dst, which = GATHER[j]
        par = s % 2
        return remote(xbuf.at[par, pl.ds(base(src, k), PARTS[k])], xbuf.at[par, pl.ds(base(dst, k), PARTS[k])],
                      ag_s.at[par, k, j], ag_r.at[par, k, j], nbr[AXES_OF[k][which]])

    def rs(s, k, j):
        par, r = s % 2, PARTS[k]
        if j == 0:
            src, dst, which = pbuf.at[par, pl.ds(base(6, k), 2 * r)], ra.at[par, pl.ds(base(2, k), 2 * r)], 0
        elif j == 1:
            src, dst, which = pbuf.at[par, pl.ds(base(4, k), 2 * r)], ra.at[par, pl.ds(base(0, k), 2 * r)], 0
        elif j == 2:
            src, dst, which = pbuf.at[par, pl.ds(base(3, k), r)], rb.at[par, pl.ds(2 * OFFS[k] + r, r)], 1
        elif j == 3:
            src, dst, which = pbuf.at[par, pl.ds(base(2, k), r)], rb.at[par, pl.ds(2 * OFFS[k], r)], 1
        else:
            src, dst, which = pbuf.at[par, pl.ds(base(1, k), r)], rc.at[par, pl.ds(OFFS[k], r)], 2
        return remote(src, dst, rs_s.at[par, k, j], rs_r.at[par, k, j], nbr[AXES_OF[k][which]])

    def tok_load(mb, k):
        return pltpu.make_async_copy(tok.at[mb, pl.ds(OFFS[k], PARTS[k])], xbuf.at[mb, pl.ds(base(0, k), PARTS[k])], t_s.at[mb, k])

    def out_store(mb, k):
        rows = pl.ds(OFFS[k], PARTS[k])
        return pltpu.make_async_copy(fin.at[mb, rows], out.at[mb, rows], o_s.at[mb, k])

    def w_local(layer):
        return [pltpu.make_async_copy(h.at[layer], v.at[pl.ds(0, 2)], wl_s.at[i]) for i, (h, v) in enumerate(((w1h, w1), (w3h, w3), (w2h, w2)))]

    def w_remote(layer):
        return [remote(h.at[layer], v.at[pl.ds(2, 2)], wr_s.at[i], wr_r.at[i], sib) for i, (h, v) in enumerate(((w1h, w1), (w3h, w3), (w2h, w2)))]

    def gate_copy(r):
        bx, by, bz = r & 1, (r >> 1) & 1, (r >> 2) & 1
        rows = pl.ds(16 * r, 16)
        return remote(tt.at[rows], gr.at[rows], g_s.at[r], g_r.at[r], dev(bx, by, bz))

    def ag_begin(s, k):
        for j in range(3):
            ag(s, k, j).start()

    def f1(s):
        for k in range(3):
            ag(s, k, 0).wait_recv()
            ag(s, k, 3).start()
            ag(s, k, 4).start()

    def f2(s):
        for k in range(3):
            ag(s, k, 1).wait_recv()
            ag(s, k, 5).start()

    def f3(s):
        for k in range(3):
            ag(s, k, 3).wait_recv()
            ag(s, k, 6).start()

    def far(s, k):
        for j in (2, 4, 5, 6):
            ag(s, k, j).wait_recv()

    def ag_sent(s):
        for k in range(3):
            for j in range(7):
                ag(s, k, j).wait_send()

    def rs_sent(s):
        for k in range(3):
            for j in range(5):
                rs(s, k, j).wait_send()

    def send_far(s, k):
        rs(s, k, 0).start()
        rs(s, k, 1).start()

    def add(s, place, k, n, src):
        rows = pl.ds(base(place, k), n)
        pbuf[s % 2, rows] = pbuf[s % 2, rows] + src

    def r1(s, k):
        r = PARTS[k]
        rs(s, k, 0).wait_recv()
        add(s, 2, k, 2 * r, ra[s % 2, pl.ds(base(2, k), 2 * r)])
        rs(s, k, 2).start()
        rs(s, k, 3).start()

    def r2(s, k):
        r = PARTS[k]
        rs(s, k, 1).wait_recv()
        add(s, 0, k, 2 * r, ra[s % 2, pl.ds(base(0, k), 2 * r)])

    def r3(s, k):
        r = PARTS[k]
        rs(s, k, 2).wait_recv()
        add(s, 1, k, r, rb[s % 2, pl.ds(2 * OFFS[k] + r, r)])
        rs(s, k, 4).start()

    def r45(s, k):
        par, r = s % 2, PARTS[k]
        rs(s, k, 3).wait_recv()
        rs(s, k, 4).wait_recv()
        rows = pl.ds(base(0, k), r)
        total = pbuf[par, rows] + rb[par, pl.ds(2 * OFFS[k], r)] + rc[par, pl.ds(OFFS[k], r)]
        new = (xbuf[par, rows].astype(F32) + ROUTE_SCALE * total).astype(BF16)
        if s < 2:
            xbuf[par, rows] = new
            ag_begin(s + 2, k)
        else:
            fin[par, pl.ds(OFFS[k], r)] = new
            out_store(par, k).start()

    def give_credit():
        for d in range(3):
            pl.semaphore_signal(credit.at[d], inc=1, device_id=nbr[d], device_id_type=MESH)

    def take_credit():
        for d in range(3):
            pl.semaphore_wait(credit.at[d], 1)

    for mb in range(2):
        for k in range(3):
            tok_load(mb, k).start()
    for cp in w_local(0):
        cp.start()
    barrier = pltpu.get_barrier_semaphore()
    for r in range(1, 8):
        pl.semaphore_signal(barrier, inc=1, device_id=dev(r & 1, (r >> 1) & 1, (r >> 2) & 1), device_id_type=MESH)
    pl.semaphore_signal(barrier, inc=1, device_id=sib, device_id_type=MESH)
    pl.semaphore_wait(barrier, 8)
    for k in range(3):
        tok_load(0, k).wait()
        ag_begin(0, k)
    for cp in w_remote(0):
        cp.start()

    lane = lax.broadcasted_iota(jnp.int32, (32, 128), 1)
    rel = lane // 16
    bx, by, bz = rel % 2, (rel // 2) % 2, rel // 4
    chip = (x + bx - 2 * x * bx) + 2 * (y + by - 2 * y * by) + 4 * (z + bz - 2 * z * bz)
    expert = 4 * chip + (lane % 4 + 2 * core) % 4
    stage_of = (lane % 16) // 4
    wanted = [jnp.where(stage_of == s, expert, -1) for s in range(STAGES)]

    def table_rows(i, _):
        acc = jnp.zeros((32, 128), F32)
        for s in range(STAGES):
            rows = pl.ds(pl.multiple_of(s * TOK + i * 32, 32), 32)
            id_blk, gt_blk = ids[rows, :], gts[rows, :]
            for j in range(8):
                acc = jnp.where(wanted[s] == id_blk[:, j:j + 1], gt_blk[:, j:j + 1], acc)
        gbuf[pl.ds(pl.multiple_of(i * 32, 32), 32), :] = acc
        return 0

    lax.fori_loop(0, TOK // 32, table_rows, 0)
    tt[...] = gbuf[pl.ds(0, TOK), :].T
    for r in range(1, 8):
        gate_copy(r).start()
    gr[pl.ds(0, 16)] = tt[pl.ds(0, 16)]

    f1(0)
    f2(0)
    f3(0)
    for k in range(3):
        tok_load(1, k).wait()
        ag_begin(1, k)
    for r in range(1, 8):
        gate_copy(r).wait()
    by_token = gr[...].T
    for k in range(3):
        for place in range(8):
            bits = bits_of(place, k)
            r = bits[0] + 2 * bits[1] + 4 * bits[2]
            piece = by_token[OFFS[k]:OFFS[k] + PARTS[k], :]
            gbuf[pl.ds(base(place, k), PARTS[k]), :] = pltpu.roll(piece, (128 - 16 * r) % 128, axis=1) if r else piece
    for cp in w_local(0) + w_remote(0):
        cp.wait()

    def after_layer_one():
        send_far(1, 2)
        ag_sent(1)
        give_credit()
        pl.semaphore_signal(wfree, inc=1, device_id=sib, device_id_type=MESH)
        for cp in w_local(1):
            cp.start()
        pl.semaphore_wait(wfree, 1)
        for cp in w_remote(1):
            cp.start()
        for k in range(3):
            r3(0, k)
        take_credit()
        for k in range(3):
            r45(0, k)
        for k in range(3):
            r1(1, k)
        f1(2)
        f2(2)
        for k in range(3):
            r2(1, k)
        f3(2)
        for cp in w_local(1) + w_remote(1):
            cp.wait()
        rs_sent(0)

    def each(step, s):
        for k in range(3):
            step(s, k)

    def begin_last():
        take_credit()
        each(r45, 1)

    plan = {
        4: [lambda: far(0, 0), lambda: f1(1)],
        5: [lambda: far(0, 1), lambda: f2(1)],
        6: [lambda: far(0, 2), lambda: send_far(0, 0), lambda: f3(1)],
        7: [lambda: send_far(0, 1)],
        8: [lambda: send_far(0, 2), lambda: ag_sent(0), give_credit],
        12: [lambda: each(r1, 0), lambda: far(1, 0)],
        13: [lambda: far(1, 1)],
        14: [lambda: far(1, 2), lambda: send_far(1, 0)],
        15: [lambda: send_far(1, 1), lambda: each(r2, 0)],
        16: [after_layer_one],
        17: [lambda: each(r3, 1)],
        18: [begin_last],
        20: [lambda: far(2, 0)],
        21: [lambda: far(2, 1), lambda: f1(3)],
        22: [lambda: far(2, 2), lambda: send_far(2, 0), lambda: f2(3)],
        23: [lambda: send_far(2, 1), lambda: f3(3)],
        24: [lambda: send_far(2, 2), lambda: ag_sent(2), lambda: rs_sent(1)],
        26: [lambda: each(r1, 2)],
        28: [lambda: far(3, 0)],
        29: [lambda: far(3, 1), lambda: each(r2, 2)],
        30: [lambda: far(3, 2), lambda: send_far(3, 0)],
        31: [lambda: send_far(3, 1), lambda: each(r3, 2)],
    }

    chunk_lane = lax.broadcasted_iota(jnp.int32, (CHUNK, 128), 1)

    def chunk(n, _):
        for when, steps in plan.items():
            @pl.when(n == when)
            def _():
                for step in steps:
                    step()
        stage = n // CHUNKS
        par = stage % 2
        rows = pl.ds(pl.multiple_of((n % CHUNKS) * CHUNK, CHUNK), CHUNK)
        x_blk = xbuf[par, rows, :]
        g_blk = gbuf[rows, :]
        for e in range(4):
            a = jnp.dot(x_blk, w1[e], preferred_element_type=F32)
            b = jnp.dot(x_blk, w3[e], preferred_element_type=F32)
            h = (jax.nn.silu(a) * b).astype(BF16)
            o = jnp.dot(h, w2[e], preferred_element_type=F32).astype(BF16).astype(F32)
            g = jnp.sum(jnp.where(chunk_lane == stage * 4 + e, g_blk, 0.0), axis=1, keepdims=True)
            term = jnp.where(g > 0.0, g * o, 0.0)
            pbuf[par, rows, :] = term if e == 0 else pbuf[par, rows, :] + term
        return 0

    lax.fori_loop(0, STAGES * CHUNKS, chunk, 0)
    send_far(3, 2)
    each(r45, 2)
    each(r1, 3)
    each(r2, 3)
    each(r3, 3)
    each(r45, 3)
    ag_sent(3)
    rs_sent(2)
    rs_sent(3)
    for mb in range(2):
        for k in range(3):
            out_store(mb, k).wait()


def solution(mesh):
    tok_spec = P(None, MESH_AXES, None)
    route_spec = P(None, None, MESH_AXES, None)
    weight_spec = P(None, MESH_AXES, None, None)

    def device_body(tokens_in, expert_ids, gate_vals, w_up1, w_up3, w_down):
        any_spec = pl.BlockSpec(memory_space=pl.ANY)
        vmem_spec = pl.BlockSpec(memory_space=pltpu.VMEM)
        dma = pltpu.SemaphoreType.DMA
        return pl.pallas_call(
            moe_kernel,
            name="moe_layers",
            out_shape=jax.ShapeDtypeStruct(tokens_in.shape, BF16),
            in_specs=[any_spec, vmem_spec, vmem_spec, any_spec, any_spec, any_spec],
            out_specs=any_spec,
            scratch_shapes=[
                pltpu.VMEM((2, 8 * TOK, HID), BF16),
                pltpu.VMEM((2, 8 * TOK, HID), F32),
                pltpu.VMEM((2, HALF, HID), F32),
                pltpu.VMEM((2, 2 * TOK, HID), F32),
                pltpu.VMEM((2, TOK, HID), F32),
                pltpu.VMEM((4, HID, FFN), BF16),
                pltpu.VMEM((4, HID, FFN), BF16),
                pltpu.VMEM((4, FFN, HID), BF16),
                pltpu.VMEM((128, TOK), F32),
                pltpu.VMEM((128, TOK), F32),
                pltpu.VMEM((8 * TOK, 128), F32),
                pltpu.VMEM((2, TOK, HID), BF16),
                dma((2, 3, 7)), dma((2, 3, 7)), dma((2, 3, 5)), dma((2, 3, 5)),
                dma((3,)), dma((3,)), dma((3,)), dma((8,)), dma((8,)), dma((2, 3)), dma((2, 3)),
                pltpu.SemaphoreType.REGULAR((3,)), pltpu.SemaphoreType.REGULAR,
            ],
            compiler_params=pltpu.CompilerParams(collective_id=0, has_side_effects=True, vmem_limit_bytes=66 * 10**6),
        )(tokens_in, expert_ids.reshape(-1, expert_ids.shape[-1]), gate_vals.reshape(-1, gate_vals.shape[-1]), w_up1, w_up3, w_down)

    return jax.shard_map(device_body, mesh=mesh, in_specs=(tok_spec, route_spec, route_spec, weight_spec, weight_spec, weight_spec), out_specs=tok_spec, check_vma=False)
```

```python
import jax
import jax.numpy as jnp
from jax import lax
from jax.experimental import pallas as pl
from jax.experimental.pallas import tpu as pltpu
from jax.sharding import PartitionSpec as P

ROUTE_SCALE = 2.5
MESH_AXES = ("ez", "ey", "ex")
MESH = pl.DeviceIdType.MESH
BF16, F32 = jnp.bfloat16, jnp.float32

TOK, HID, FFN = 256, 1024, 512
PART = TOK // 2
CHUNK = 256
PIECES = 4

AXES1 = (((0, 2, 1), (1, 2, 0)), ((0, 2, 1), (1, 0, 2)))
AXES2 = ((0, 1), (1, 0))
GATHER1 = ((0, 2, 1), (0, 1, 2), (0, 4, 0), (2, 3, 2), (2, 6, 0), (1, 5, 0), (3, 7, 0))
GATHER2 = ((0, 1, 1), (0, 2, 0), (1, 3, 0))


def base1(place, k):
    return (place // 4) * 4 * TOK + k * 4 * PART + (place % 4) * PART


def base2(place, k):
    return (place // 2) * 2 * TOK + k * 2 * PART + (place % 2) * PART


def block_of(place, axes):
    n = len(axes)
    return sum(((place >> (n - 1 - i)) & 1) << axis for i, axis in enumerate(axes))


def moe_kernel(tok, ids, gts, w1h, w3h, w2h, out, f1h, f3h, f2h, xbuf, x2, pbuf, ra, rb, rc, w1, w3, w2, tt, gr, gbuf, g2, fin,
               ag_s, ag_r, rs_s, rs_r, bg_s, bg_r, bs_s, bs_r, wl_s, wr_s, wr_r, wb_s, wb_r, z_s, z_r, fw_s, fw_r, g_s, g_r, t_s, o_s):
    z, y, ex = (lax.axis_index(name) for name in MESH_AXES)
    x, core = ex // 2, ex % 2

    def turned(bu, bv):
        return bu + core * (bv - bu), bv + core * (bu - bv)

    def dev(bu, bv, bz):
        bx, by = turned(bu, bv)
        return (z + bz - 2 * z * bz, y + by - 2 * y * by, (x + bx - 2 * x * bx) * 2 + core)

    nbr = (dev(1, 0, 0), dev(0, 1, 0), dev(0, 0, 1))
    sib = (z, y, x * 2 + 1 - core)

    def remote(src, dst, ss, rs, to):
        return pltpu.make_async_remote_copy(src_ref=src, dst_ref=dst, send_sem=ss, recv_sem=rs, device_id=to, device_id_type=MESH)

    def ag(s, k, j):
        src, dst, which = GATHER1[j]
        return remote(xbuf.at[s, pl.ds(base1(src, k), PART)], xbuf.at[s, pl.ds(base1(dst, k), PART)],
                      ag_s.at[s, k, j], ag_r.at[s, k, j], nbr[AXES1[s][k][which]])

    def rs(s, k, j):
        if j < 2:
            src, dst, which = pbuf.at[s, pl.ds(base1(6 - 2 * j, k), 2 * PART)], ra.at[s, pl.ds((4 * k + 2 - 2 * j) * PART, 2 * PART)], 0
        elif j < 4:
            src, dst, which = pbuf.at[s, pl.ds(base1(7 - 2 * j, k), PART)], rb.at[s, pl.ds((2 * k + 3 - j) * PART, PART)], 2
        else:
            src, dst, which = pbuf.at[s, pl.ds(base1(2, k), PART)], rc.at[s, pl.ds(k * PART, PART)], 1
        return remote(src, dst, rs_s.at[s, k, j], rs_r.at[s, k, j], nbr[AXES1[s][k][which]])

    def bg(s, k, j):
        src, dst, which = GATHER2[j]
        return remote(x2.at[s, pl.ds(base2(src, k), PART)], x2.at[s, pl.ds(base2(dst, k), PART)],
                      bg_s.at[s, k, j], bg_r.at[s, k, j], nbr[AXES2[k][which]])

    def bs(s, k, j):
        if j < 2:
            src, dst, which = pbuf.at[s, pl.ds(base2(3 - j, k), PART)], ra.at[s, pl.ds((4 * k + 1 - j) * PART, PART)], 0
        else:
            src, dst, which = pbuf.at[s, pl.ds(base2(1, k), PART)], rb.at[s, pl.ds(2 * k * PART, PART)], 1
        return remote(src, dst, bs_s.at[s, k, j], bs_r.at[s, k, j], nbr[AXES2[k][which]])

    def tok_load(mb, k):
        return pltpu.make_async_copy(tok.at[mb, pl.ds(k * PART, PART)], xbuf.at[mb, pl.ds(base1(0, k), PART)], t_s.at[mb, k])

    def out_store(mb, k):
        rows = pl.ds(k * PART, PART)
        return pltpu.make_async_copy(fin.at[mb, rows], out.at[mb, rows], o_s.at[mb, k])

    held = ((w1h, f1h, w1), (w3h, f3h, w3), (w2h, f2h, w2))

    def w_first_local():
        return [pltpu.make_async_copy(h.at[0, e], v.at[e], wl_s.at[e, i]) for e in range(2) for i, (h, _, v) in enumerate(held)]

    def w_first_remote():
        return [remote(h.at[0], v.at[pl.ds(2, 2)], wr_s.at[i], wr_r.at[i], sib) for i, (h, _, v) in enumerate(held)]

    def w_second_swap():
        return [remote(h.at[1], f.at[pl.ds(0, 2)], wb_s.at[i], wb_r.at[i], sib) for i, (h, f, _) in enumerate(held)]

    def w_piece(p):
        e, i, q = p // (3 * PIECES), (p // PIECES) % 3, p % PIECES
        h, f, _ = held[i]
        rows = pl.ds(q * (h.shape[2] // PIECES), h.shape[2] // PIECES)
        return remote(h.at[1, e, rows], f.at[2 + e, rows], z_s.at[p], z_r.at[p], nbr[2])

    def w_forward(e):
        return [remote(f.at[2 + e], f.at[4 + e], fw_s.at[e, i], fw_r.at[e, i], sib) for i, (_, f, _) in enumerate(held)]

    def w_load(zc, slot):
        if zc:
            srcs = [f.at[2 + slot] for _, f, _ in held]
        else:
            srcs = [h.at[1, slot] if slot < 2 else f.at[slot - 2] for h, f, _ in held]
        return [pltpu.make_async_copy(src, held[i][2].at[slot], wl_s.at[slot, i]) for i, src in enumerate(srcs)]

    def start(copies):
        for cp in copies:
            cp.start()

    def wait(copies):
        for cp in copies:
            cp.wait()

    def wait_recv(copies):
        for cp in copies:
            cp.wait_recv()

    def pieces_in(e):
        wait_recv([w_piece(p) for p in range(e * 3 * PIECES, (e + 1) * 3 * PIECES)])

    fed = [0]

    def feed(n):
        while n and fed[0] < 6 * PIECES:
            w_piece(fed[0]).start()
            fed[0] += 1
            n -= 1

    gate_rows = [(16 * r, 16, r) for r in (1, 2, 3)] + [(16 * (r + 4) + 8, 8, r) for r in (1, 2, 3)] + [(16 * r, 8, r) for r in (4, 5, 6, 7)]

    def gate_copies():
        return [remote(tt.at[pl.ds(row, n)], gr.at[pl.ds(row, n)], g_s.at[i], g_r.at[i], dev(r & 1, (r >> 1) & 1, r >> 2))
                for i, (row, n, r) in enumerate(gate_rows)]

    def ag_begin(s, *js):
        for j in js:
            for k in range(2):
                ag(s, k, j).start()

    def f1(s):
        for k in range(2):
            ag(s, k, 0).wait_recv()
            ag(s, k, 3).start()
            ag(s, k, 4).start()

    def f2(s):
        for k in range(2):
            ag(s, k, 1).wait_recv()
            ag(s, k, 5).start()

    def f3(s):
        for k in range(2):
            ag(s, k, 3).wait_recv()
            ag(s, k, 6).start()

    def far(s, k):
        for j in (2, 4, 5, 6):
            ag(s, k, j).wait_recv()

    def add(s, row, n, src):
        rows = pl.ds(row, n)
        pbuf[s, rows] = pbuf[s, rows] + src

    def r1(s):
        for k in range(2):
            rs(s, k, 0).wait_recv()
            add(s, base1(2, k), 2 * PART, ra[s, pl.ds((4 * k + 2) * PART, 2 * PART)])
            rs(s, k, 2).start()

    def r2(s):
        for k in range(2):
            rs(s, k, 1).wait_recv()
            add(s, base1(0, k), 2 * PART, ra[s, pl.ds(4 * k * PART, 2 * PART)])
            rs(s, k, 3).start()

    def r3(s):
        for k in range(2):
            rs(s, k, 2).wait_recv()
            add(s, base1(2, k), PART, rb[s, pl.ds((2 * k + 1) * PART, PART)])
            rs(s, k, 4).start()

    def r45(s):
        for k in range(2):
            rs(s, k, 3).wait_recv()
            rs(s, k, 4).wait_recv()
            rows = pl.ds(base1(0, k), PART)
            total = pbuf[s, rows] + rb[s, pl.ds(2 * k * PART, PART)] + rc[s, pl.ds(k * PART, PART)]
            x2[s, pl.ds(base2(0, k), PART)] = (xbuf[s, rows].astype(F32) + ROUTE_SCALE * total).astype(BF16)
            bg(s, k, 0).start()
            bg(s, k, 1).start()

    def clear(s):
        for k in range(2):
            for j in range(5):
                rs(s, k, j).wait_send()
        pbuf[s, pl.ds(0, 4 * TOK)] = jnp.zeros((4 * TOK, HID), F32)

    def g1(s):
        for k in range(2):
            bg(s, k, 0).wait_recv()
            bg(s, k, 2).start()

    def g_far(s):
        for k in range(2):
            bg(s, k, 1).wait_recv()
            bg(s, k, 2).wait_recv()

    def b_far(s):
        for j in range(2):
            for k in range(2):
                bs(s, k, j).start()

    def b1(s):
        for k in range(2):
            bs(s, k, 0).wait_recv()
            add(s, base2(1, k), PART, ra[s, pl.ds((4 * k + 1) * PART, PART)])
            bs(s, k, 2).start()

    def b2(s):
        for k in range(2):
            bs(s, k, 1).wait_recv()
            bs(s, k, 2).wait_recv()
            rows = pl.ds(base2(0, k), PART)
            total = pbuf[s, rows] + ra[s, pl.ds(4 * k * PART, PART)] + rb[s, pl.ds(2 * k * PART, PART)]
            fin[s, pl.ds(k * PART, PART)] = (x2[s, rows].astype(F32) + ROUTE_SCALE * total).astype(BF16)
            out_store(s, k).start()

    for mb in range(2):
        for k in range(2):
            tok_load(mb, k).start()
    start(w_first_local())
    barrier = pltpu.get_barrier_semaphore()
    for r in range(1, 8):
        pl.semaphore_signal(barrier, inc=1, device_id=dev(r & 1, (r >> 1) & 1, (r >> 2) & 1), device_id_type=MESH)
    pl.semaphore_signal(barrier, inc=1, device_id=sib, device_id_type=MESH)
    pl.semaphore_wait(barrier, 8)
    wait([tok_load(0, 0), tok_load(0, 1)])
    ag_begin(0, 0, 2, 1)
    wait([tok_load(1, 0), tok_load(1, 1)])
    ag_begin(1, 0)
    start(w_first_remote())

    row = lax.broadcasted_iota(jnp.int32, (128, TOK), 0)
    rel = row // 16
    bx, by = turned(rel % 2, (rel // 2) % 2)
    bz = rel // 4
    chip = (x + bx - 2 * x * bx) + 2 * (y + by - 2 * y * by) + 4 * (z + bz - 2 * z * bz)
    expert = 4 * chip + (row % 4 + 2 * core) % 4
    table = jnp.zeros((128, TOK), F32)
    for s in range(4):
        wanted = jnp.where((row % 16) // 4 == s, expert, -1)
        for j in range(8):
            i = 8 * s + j
            table = jnp.where(wanted == ids[i:i + 1, :], gts[i:i + 1, :], table)
    tt[...] = table
    start(gate_copies())
    gr[pl.ds(0, 16)] = tt[pl.ds(0, 16)]
    gr[pl.ds(72, 8)] = tt[pl.ds(72, 8)]

    f1(0)
    f2(0)
    feed(2)
    wait(gate_copies())
    by_token = gr[...].T
    low = lax.broadcasted_iota(jnp.int32, (PART, 128), 1)
    for k in range(2):
        piece = by_token[k * PART:(k + 1) * PART, :]

        def lanes_from(lane, to):
            return pltpu.roll(piece, (to - lane) % 128, axis=1) if lane != to else piece

        for place in range(8):
            r0, r1_ = block_of(place, AXES1[0][k]), block_of(place, AXES1[1][k])
            gbuf[pl.ds(base1(place, k), PART), :] = jnp.where(low < 4, lanes_from(16 * r0, 0), lanes_from(16 * r1_, 0))
        for place in range(4):
            r = block_of(place, AXES2[k])
            g2[pl.ds(base2(place, k), PART), :] = jnp.where(low < 8, lanes_from(16 * r + 8, 0), lanes_from(16 * (r + 4) + 8, 8))
    wait(w_first_local() + w_first_remote())

    lane = lax.broadcasted_iota(jnp.int32, (CHUNK, 128), 1)

    def weighted(x_blk, g_blk, column, slot):
        a = jnp.dot(x_blk, w1[slot], preferred_element_type=F32)
        b = jnp.dot(x_blk, w3[slot], preferred_element_type=F32)
        h = (jax.nn.silu(a) * b).astype(BF16)
        o = jnp.dot(h, w2[slot], preferred_element_type=F32).astype(BF16).astype(F32)
        g = jnp.sum(jnp.where(lane == column, g_blk, 0.0), axis=1, keepdims=True)
        return jnp.where(g > 0.0, g * o, 0.0)

    def hooks(n, plan):
        for when in sorted(plan):
            @pl.when(n == when)
            def _():
                for step in plan[when]:
                    step()

    def send(s, k, j):
        return lambda: rs(s, k, j).start()

    plan1 = {n: [lambda: feed(1)] for n in range(16)}
    plan1[1] += [lambda: f3(0), lambda: ag_begin(1, 2, 1), lambda: f1(1)]
    plan1[4] += [lambda: far(0, 0)]
    plan1[5] += [lambda: f2(1)]
    plan1[6] += [lambda: f3(1), send(0, 0, 0), send(0, 0, 1), lambda: far(0, 1)]
    plan1[7] += [send(0, 1, 0)]
    plan1[8] += [send(0, 1, 1)]
    plan1[9] += [lambda: start(w_second_swap())]
    plan1[12] += [lambda: far(1, 0)]
    plan1[14] += [lambda: far(1, 1)]

    def layer1(n, _):
        hooks(n, plan1)
        s = n // 8
        c = n % 8
        c = c + (c // 4) * (1 - 2 * (c % 2))
        rows = pl.ds(pl.multiple_of(c * CHUNK, CHUNK), CHUNK)
        x_blk, g_blk = xbuf[s, rows, :], gbuf[rows, :]
        for e in range(4):
            term = weighted(x_blk, g_blk, s * 4 + e, e)
            pbuf[s, rows, :] = term if e == 0 else pbuf[s, rows, :] + term
        return 0

    lax.fori_loop(0, 16, layer1, 0)

    start(w_load(0, 0) + w_load(0, 1))
    r1(0)
    wait_recv(w_second_swap())
    start(w_load(0, 2) + w_load(0, 3))
    pieces_in(0)
    start(w_forward(0))
    r2(0)
    for k in range(2):
        rs(1, k, 0).start()
    r3(0)
    feed(1)
    r45(0)
    r1(1)
    feed(2)
    g1(0)
    for k in range(2):
        rs(1, k, 1).start()
    clear(0)
    r3(1)
    feed(2)
    for slot in range(4):
        wait(w_load(0, slot))
    g_far(0)

    def unit(s, half, zc, slot):
        for part in range(2):
            rows = pl.ds(pl.multiple_of(half * 2 * TOK + part * CHUNK, CHUNK), CHUNK)
            pbuf[s, rows, :] += weighted(x2[s, rows, :], g2[rows, :], zc * 8 + s * 4 + slot, slot)

    order = (0, 2, 1, 3)

    def load(zc, slot):
        return lambda: start(w_load(zc, slot))

    def loaded(zc, slot):
        return lambda: wait(w_load(zc, slot))

    plan2 = {
        2: [load(1, 0)],
        4: [lambda: wait_recv(w_forward(0)), load(1, 2)],
        8: [loaded(1, 0), lambda: r2(1), lambda: feed(24)],
        10: [loaded(1, 2)],
        11: [lambda: r45(1)],
    }

    def second_a(m, _):
        hooks(m, plan2)
        i = m // 2
        unit(0, 1 - m % 2, i // 4, (i % 2) * 2 + (i % 4) // 2)
        return 0

    lax.fori_loop(0, 12, second_a, 0)
    pieces_in(1)
    start(w_forward(1))
    load(1, 1)()
    clear(1)
    loaded(1, 1)()

    def arrived():
        wait_recv(w_forward(1))
        start(w_load(1, 3))
        g1(1)
        wait(w_load(1, 3))

    plan3 = {1: [arrived], 2: [lambda: b_far(0)]}

    def second_b(m, _):
        hooks(m, plan3)
        unit(0, 1 - m // 2, 1, 1 + 2 * (m % 2))
        return 0

    lax.fori_loop(0, 4, second_b, 0)
    g_far(1)

    plan4 = {}
    for i in range(4):
        plan4.setdefault(i + 1, []).append(load(0, order[i]))
        plan4.setdefault(i + 9, []).append(load(1, order[i]))
        plan4.setdefault(i + 4, []).append(loaded(0, order[i]))
        plan4.setdefault(i + 12, []).append(loaded(1, order[i]))
    plan4[6].append(lambda: b1(0))
    plan4.setdefault(8, []).append(lambda: b_far(1))

    def second_c(m, _):
        hooks(m, plan4)
        q, j = m // 4, m % 4
        unit(1, 1 - q // 2, 1 - ((q + 1) // 2) % 2, (j % 2) * 2 + j // 2)
        return 0

    lax.fori_loop(0, 16, second_c, 0)
    b2(0)
    b1(1)
    b2(1)
    for s in range(2):
        for k in range(2):
            for j in range(7):
                ag(s, k, j).wait_send()
            for j in range(3):
                bg(s, k, j).wait_send()
                bs(s, k, j).wait_send()
    for cp in w_second_swap() + w_forward(0) + w_forward(1) + [w_piece(p) for p in range(6 * PIECES)]:
        cp.wait_send()
    for mb in range(2):
        for k in range(2):
            out_store(mb, k).wait()


def solution(mesh):
    tok_spec = P(None, MESH_AXES, None)
    route_spec = P(None, None, MESH_AXES, None)
    weight_spec = P(None, MESH_AXES, None, None)

    def device_body(tokens_in, expert_ids, gate_vals, w_up1, w_up3, w_down):
        any_spec = pl.BlockSpec(memory_space=pl.ANY)
        vmem_spec = pl.BlockSpec(memory_space=pltpu.VMEM)
        dma = pltpu.SemaphoreType.DMA

        def by_slot(route):
            return jnp.swapaxes(route, 2, 3).reshape(-1, route.shape[2])

        return pl.pallas_call(
            moe_kernel,
            name="moe_layers",
            out_shape=[
                jax.ShapeDtypeStruct(tokens_in.shape, BF16),
                jax.ShapeDtypeStruct((6, HID, FFN), BF16),
                jax.ShapeDtypeStruct((6, HID, FFN), BF16),
                jax.ShapeDtypeStruct((6, FFN, HID), BF16),
            ],
            in_specs=[any_spec, vmem_spec, vmem_spec, any_spec, any_spec, any_spec],
            out_specs=[any_spec] * 4,
            scratch_shapes=[
                pltpu.VMEM((2, 8 * TOK, HID), BF16),
                pltpu.VMEM((2, 4 * TOK, HID), BF16),
                pltpu.VMEM((2, 8 * TOK, HID), F32),
                pltpu.VMEM((2, 4 * TOK, HID), F32),
                pltpu.VMEM((2, 2 * TOK, HID), F32),
                pltpu.VMEM((2, TOK, HID), F32),
                pltpu.VMEM((4, HID, FFN), BF16),
                pltpu.VMEM((4, HID, FFN), BF16),
                pltpu.VMEM((4, FFN, HID), BF16),
                pltpu.VMEM((128, TOK), F32),
                pltpu.VMEM((128, TOK), F32),
                pltpu.VMEM((8 * TOK, 128), F32),
                pltpu.VMEM((4 * TOK, 128), F32),
                pltpu.VMEM((2, TOK, HID), BF16),
                dma((2, 2, 7)), dma((2, 2, 7)), dma((2, 2, 5)), dma((2, 2, 5)),
                dma((2, 2, 3)), dma((2, 2, 3)), dma((2, 2, 3)), dma((2, 2, 3)),
                dma((4, 3)), dma((3,)), dma((3,)), dma((3,)), dma((3,)),
                dma((6 * PIECES,)), dma((6 * PIECES,)), dma((2, 3)), dma((2, 3)), dma((10,)), dma((10,)), dma((2, 2)), dma((2, 2)),
            ],
            compiler_params=pltpu.CompilerParams(collective_id=0, has_side_effects=True, vmem_limit_bytes=66 * 10**6),
        )(tokens_in, by_slot(expert_ids), by_slot(gate_vals), w_up1, w_up3, w_down)[0]

    return jax.shard_map(device_body, mesh=mesh, in_specs=(tok_spec, route_spec, route_spec, weight_spec, weight_spec, weight_spec), out_specs=tok_spec, check_vma=False)
```

```python
import jax
import jax.numpy as jnp
from jax import lax
from jax.experimental import pallas as pl
from jax.experimental.pallas import tpu as pltpu
from jax.sharding import PartitionSpec as P

ROUTE_SCALE = 2.5
MESH_AXES = ("ez", "ey", "ex")
MESH = pl.DeviceIdType.MESH
BF16, F32 = jnp.bfloat16, jnp.float32

TOK, HID, FFN = 256, 1024, 512
N1, N2 = 4, 2
ROW1, PART = TOK // N1, TOK // N2
CHUNK = 256
PIECES = 4

AXES1 = (((0, 2, 1), (1, 2, 0)) * 2, ((0, 2, 1), (1, 2, 0), (0, 1, 2), (1, 0, 2)))
AXES2 = ((0, 1), (1, 0))
GATHER1 = ((0, 2, 1), (0, 1, 2), (0, 4, 0), (2, 3, 2), (2, 6, 0), (1, 5, 0), (3, 7, 0))
GATHER2 = ((0, 1, 1), (0, 2, 0), (1, 3, 0))


def base1(place, k):
    return (place // 4) * 4 * TOK + k * 4 * ROW1 + (place % 4) * ROW1


def base2(place, k):
    return (place // 2) * 2 * TOK + k * 2 * PART + (place % 2) * PART


def block_of(place, axes):
    n = len(axes)
    return sum(((place >> (n - 1 - i)) & 1) << axis for i, axis in enumerate(axes))


def moe_kernel(tok, ids, gts, w1h, w3h, w2h, out, f1h, f3h, f2h, xbuf, x2, pbuf, ra, rb, rc, w1, w3, w2, tt, gr, gbuf, g2, fin,
               ag_s, ag_r, rs_s, rs_r, bg_s, bg_r, bs_s, bs_r, wl_s, wr_s, wr_r, wb_s, wb_r, z_s, z_r, fw_s, fw_r, g_s, g_r, t_s, o_s):
    z, y, ex = (lax.axis_index(name) for name in MESH_AXES)
    x, core = ex // 2, ex % 2

    def turned(bu, bv):
        return bu + core * (bv - bu), bv + core * (bu - bv)

    def dev(bu, bv, bz):
        bx, by = turned(bu, bv)
        return (z + bz - 2 * z * bz, y + by - 2 * y * by, (x + bx - 2 * x * bx) * 2 + core)

    nbr = (dev(1, 0, 0), dev(0, 1, 0), dev(0, 0, 1))
    sib = (z, y, x * 2 + 1 - core)

    def remote(src, dst, ss, rs, to):
        return pltpu.make_async_remote_copy(src_ref=src, dst_ref=dst, send_sem=ss, recv_sem=rs, device_id=to, device_id_type=MESH)

    def ag(s, k, j):
        src, dst, which = GATHER1[j]
        return remote(xbuf.at[s, pl.ds(base1(src, k), ROW1)], xbuf.at[s, pl.ds(base1(dst, k), ROW1)],
                      ag_s.at[s, k, j], ag_r.at[s, k, j], nbr[AXES1[s][k][which]])

    def rs(s, k, j):
        if j < 2:
            src, dst, which = pbuf.at[s, pl.ds(base1(6 - 2 * j, k), 2 * ROW1)], ra.at[s, pl.ds((4 * k + 2 - 2 * j) * ROW1, 2 * ROW1)], 0
        elif j < 4:
            src, dst, which = pbuf.at[s, pl.ds(base1(7 - 2 * j, k), ROW1)], rb.at[s, pl.ds((2 * k + 3 - j) * ROW1, ROW1)], 2
        else:
            src, dst, which = pbuf.at[s, pl.ds(base1(2, k), ROW1)], rc.at[s, pl.ds(k * ROW1, ROW1)], 1
        return remote(src, dst, rs_s.at[s, k, j], rs_r.at[s, k, j], nbr[AXES1[s][k][which]])

    def bg(s, k, j):
        src, dst, which = GATHER2[j]
        return remote(x2.at[s, pl.ds(base2(src, k), PART)], x2.at[s, pl.ds(base2(dst, k), PART)],
                      bg_s.at[s, k, j], bg_r.at[s, k, j], nbr[AXES2[k][which]])

    def bs(s, k, j):
        if j < 2:
            src, dst, which = pbuf.at[s, pl.ds(base2(3 - j, k), PART)], ra.at[s, pl.ds((4 * k + 1 - j) * PART, PART)], 0
        else:
            src, dst, which = pbuf.at[s, pl.ds(base2(1, k), PART)], rb.at[s, pl.ds(2 * k * PART, PART)], 1
        return remote(src, dst, bs_s.at[s, k, j], bs_r.at[s, k, j], nbr[AXES2[k][which]])

    def tok_load(mb):
        return [pltpu.make_async_copy(tok.at[mb, pl.ds(k * ROW1, ROW1)], xbuf.at[mb, pl.ds(base1(0, k), ROW1)], t_s.at[mb, k]) for k in range(N1)]

    def out_store(mb, k):
        rows = pl.ds(k * PART, PART)
        return pltpu.make_async_copy(fin.at[mb, rows], out.at[mb, rows], o_s.at[mb, k])

    held = ((w1h, f1h, w1), (w3h, f3h, w3), (w2h, f2h, w2))

    def w_first_local():
        return [pltpu.make_async_copy(h.at[0, e], v.at[e], wl_s.at[e, i]) for e in range(2) for i, (h, _, v) in enumerate(held)]

    def w_first_remote():
        return [remote(h.at[0], v.at[pl.ds(2, 2)], wr_s.at[i], wr_r.at[i], sib) for i, (h, _, v) in enumerate(held)]

    def w_second_swap():
        return [remote(h.at[1], f.at[pl.ds(0, 2)], wb_s.at[i], wb_r.at[i], sib) for i, (h, f, _) in enumerate(held)]

    def w_piece(p):
        e, i, q = p // (3 * PIECES), (p // PIECES) % 3, p % PIECES
        h, f, _ = held[i]
        rows = pl.ds(q * (h.shape[2] // PIECES), h.shape[2] // PIECES)
        return remote(h.at[1, e, rows], f.at[2 + e, rows], z_s.at[p], z_r.at[p], nbr[2])

    def w_forward(e):
        return [remote(f.at[2 + e], f.at[4 + e], fw_s.at[e, i], fw_r.at[e, i], sib) for i, (_, f, _) in enumerate(held)]

    def w_load(zc, slot):
        if zc:
            srcs = [f.at[2 + slot] for _, f, _ in held]
        else:
            srcs = [h.at[1, slot] if slot < 2 else f.at[slot - 2] for h, f, _ in held]
        return [pltpu.make_async_copy(src, held[i][2].at[slot], wl_s.at[slot, i]) for i, src in enumerate(srcs)]

    def start(copies):
        for cp in copies:
            cp.start()

    def wait(copies):
        for cp in copies:
            cp.wait()

    def wait_recv(copies):
        for cp in copies:
            cp.wait_recv()

    def pieces_in(e):
        wait_recv([w_piece(p) for p in range(e * 3 * PIECES, (e + 1) * 3 * PIECES)])

    fed = [0]

    def feed(n):
        while n and fed[0] < 6 * PIECES:
            w_piece(fed[0]).start()
            fed[0] += 1
            n -= 1

    gate_rows = [(16 * r, 16, r) for r in (1, 2, 3)] + [(16 * (r + 4) + 8, 8, r) for r in (1, 2, 3)] + [(16 * r, 8, r) for r in (4, 5, 6, 7)]

    def gate_copies():
        return [remote(tt.at[pl.ds(row, n)], gr.at[pl.ds(row, n)], g_s.at[i], g_r.at[i], dev(r & 1, (r >> 1) & 1, r >> 2))
                for i, (row, n, r) in enumerate(gate_rows)]

    def ag_begin(s, *js):
        for j in js:
            for k in range(N1):
                ag(s, k, j).start()

    def f1(s):
        for k in range(N1):
            ag(s, k, 0).wait_recv()
            ag(s, k, 3).start()
            ag(s, k, 4).start()

    def f2(s):
        for k in range(N1):
            ag(s, k, 1).wait_recv()
            ag(s, k, 5).start()

    def f3(s, k):
        ag(s, k, 3).wait_recv()
        ag(s, k, 6).start()

    def far(s, k):
        for j in (2, 4, 5, 6):
            ag(s, k, j).wait_recv()

    def add(s, row, n, src):
        rows = pl.ds(row, n)
        pbuf[s, rows] = pbuf[s, rows] + src

    def r1(s):
        for k in range(N1):
            rs(s, k, 0).wait_recv()
            add(s, base1(2, k), 2 * ROW1, ra[s, pl.ds((4 * k + 2) * ROW1, 2 * ROW1)])
            rs(s, k, 2).start()

    def r2(s):
        for k in range(N1):
            rs(s, k, 1).wait_recv()
            add(s, base1(0, k), 2 * ROW1, ra[s, pl.ds(4 * k * ROW1, 2 * ROW1)])
            rs(s, k, 3).start()

    def r3(s):
        for k in range(N1):
            rs(s, k, 2).wait_recv()
            add(s, base1(2, k), ROW1, rb[s, pl.ds((2 * k + 1) * ROW1, ROW1)])
            rs(s, k, 4).start()

    def r45(s):
        for k in range(N1):
            rs(s, k, 3).wait_recv()
            rs(s, k, 4).wait_recv()
            rows = pl.ds(base1(0, k), ROW1)
            total = pbuf[s, rows] + rb[s, pl.ds(2 * k * ROW1, ROW1)] + rc[s, pl.ds(k * ROW1, ROW1)]
            into = base2(0, k * N2 // N1) + (k * ROW1) % PART
            x2[s, pl.ds(into, ROW1)] = (xbuf[s, rows].astype(F32) + ROUTE_SCALE * total).astype(BF16)
            if (k + 1) * ROW1 % PART == 0:
                bg(s, k * N2 // N1, 0).start()
                bg(s, k * N2 // N1, 1).start()

    def clear(s):
        for k in range(N1):
            for j in range(5):
                rs(s, k, j).wait_send()
        pbuf[s, pl.ds(0, 4 * TOK)] = jnp.zeros((4 * TOK, HID), F32)

    def g1(s):
        for k in range(2):
            bg(s, k, 0).wait_recv()
            bg(s, k, 2).start()

    def g_far(s):
        for k in range(2):
            bg(s, k, 1).wait_recv()
            bg(s, k, 2).wait_recv()

    def b_far(s):
        for j in range(2):
            for k in range(2):
                bs(s, k, j).start()

    def b1(s):
        for k in range(2):
            bs(s, k, 0).wait_recv()
            add(s, base2(1, k), PART, ra[s, pl.ds((4 * k + 1) * PART, PART)])
            bs(s, k, 2).start()

    def b2(s):
        for k in range(2):
            bs(s, k, 1).wait_recv()
            bs(s, k, 2).wait_recv()
            rows = pl.ds(base2(0, k), PART)
            total = pbuf[s, rows] + ra[s, pl.ds(4 * k * PART, PART)] + rb[s, pl.ds(2 * k * PART, PART)]
            fin[s, pl.ds(k * PART, PART)] = (x2[s, rows].astype(F32) + ROUTE_SCALE * total).astype(BF16)
            out_store(s, k).start()

    start(tok_load(0) + tok_load(1))
    start(w_first_local())
    barrier = pltpu.get_barrier_semaphore()
    for r in range(1, 8):
        pl.semaphore_signal(barrier, inc=1, device_id=dev(r & 1, (r >> 1) & 1, (r >> 2) & 1), device_id_type=MESH)
    pl.semaphore_signal(barrier, inc=1, device_id=sib, device_id_type=MESH)
    pl.semaphore_wait(barrier, 8)
    wait(tok_load(0))
    ag_begin(0, 0, 2, 1)
    wait(tok_load(1))
    ag_begin(1, 0)
    start(w_first_remote())

    row = lax.broadcasted_iota(jnp.int32, (128, TOK), 0)
    rel = row // 16
    bx, by = turned(rel % 2, (rel // 2) % 2)
    bz = rel // 4
    chip = (x + bx - 2 * x * bx) + 2 * (y + by - 2 * y * by) + 4 * (z + bz - 2 * z * bz)
    expert = 4 * chip + (row % 4 + 2 * core) % 4
    table = jnp.zeros((128, TOK), F32)
    for s in range(4):
        wanted = jnp.where((row % 16) // 4 == s, expert, -1)
        for j in range(8):
            i = 8 * s + j
            table = jnp.where(wanted == ids[i:i + 1, :], gts[i:i + 1, :], table)
    tt[...] = table
    start(gate_copies())
    gr[pl.ds(0, 16)] = tt[pl.ds(0, 16)]
    gr[pl.ds(72, 8)] = tt[pl.ds(72, 8)]

    f1(0)
    f2(0)
    feed(2)
    wait(gate_copies())
    by_token = gr[...].T

    def lanes(piece, first, second, cut):
        spot = lax.broadcasted_iota(jnp.int32, piece.shape, 1)
        return jnp.where(spot < cut, pltpu.roll(piece, (128 - first) % 128, axis=1), pltpu.roll(piece, (cut + 128 - second) % 128, axis=1))

    for k in range(N1):
        for place in range(8):
            r_0, r_1 = block_of(place, AXES1[0][k]), block_of(place, AXES1[1][k])
            gbuf[pl.ds(base1(place, k), ROW1), :] = lanes(by_token[k * ROW1:(k + 1) * ROW1, :], 16 * r_0, 16 * r_1 + 4, 4)
    for k in range(N2):
        for place in range(4):
            r = block_of(place, AXES2[k])
            g2[pl.ds(base2(place, k), PART), :] = lanes(by_token[k * PART:(k + 1) * PART, :], 16 * r + 8, 16 * (r + 4) + 8, 8)
    wait(w_first_local() + w_first_remote())

    lane = lax.broadcasted_iota(jnp.int32, (CHUNK, 128), 1)

    def weighted(x_blk, g_blk, column, slot):
        a = jnp.dot(x_blk, w1[slot], preferred_element_type=F32)
        b = jnp.dot(x_blk, w3[slot], preferred_element_type=F32)
        h = (jax.nn.silu(a) * b).astype(BF16)
        o = jnp.dot(h, w2[slot], preferred_element_type=F32).astype(BF16).astype(F32)
        g = jnp.sum(jnp.where(lane == column, g_blk, 0.0), axis=1, keepdims=True)
        return jnp.where(g > 0.0, g * o, 0.0)

    def hooks(n, plan):
        for when in sorted(plan):
            @pl.when(n == when)
            def _():
                for step in plan[when]:
                    step()

    def send(k):
        return lambda: start([rs(0, k, 0), rs(0, k, 1)])

    plan1 = {n: [lambda: feed(1)] for n in range(16)}
    plan1[0] += [lambda: f3(0, 0)]
    plan1[1] += [lambda: f3(0, 1), lambda: f3(0, 2), lambda: f3(0, 3), lambda: ag_begin(1, 2, 1), lambda: f1(1)]
    plan1[4] += [lambda: far(0, 0)]
    plan1[5] += [lambda: far(0, 1), lambda: f2(1)]
    plan1[6] += [lambda: far(0, 2)] + [lambda k=k: f3(1, k) for k in range(N1)] + [send(0), send(1)]
    plan1[7] += [lambda: far(0, 3), send(2)]
    plan1[8] += [send(3)]
    plan1[9] += [lambda: start(w_second_swap())]
    for k in range(N1):
        plan1[12 + k] += [lambda k=k: far(1, k)]

    def layer1(n, _):
        hooks(n, plan1)
        s = n // 8
        rows = pl.ds(pl.multiple_of((n % 8) * CHUNK, CHUNK), CHUNK)
        x_blk, g_blk = xbuf[s, rows, :], gbuf[rows, :]
        for e in range(4):
            term = weighted(x_blk, g_blk, s * 4 + e, e)
            pbuf[s, rows, :] = term if e == 0 else pbuf[s, rows, :] + term
        return 0

    lax.fori_loop(0, 16, layer1, 0)

    start(w_load(0, 0) + w_load(0, 1))
    r1(0)
    wait_recv(w_second_swap())
    start(w_load(0, 2) + w_load(0, 3))
    pieces_in(0)
    start(w_forward(0))
    r2(0)
    start([rs(1, k, 0) for k in range(N1)])
    r3(0)
    feed(1)
    r45(0)
    r1(1)
    feed(2)
    g1(0)
    start([rs(1, k, 1) for k in range(N1)])
    clear(0)
    r3(1)
    feed(2)
    for slot in range(4):
        wait(w_load(0, slot))
    g_far(0)

    def unit(s, half, zc, slot):
        for part in range(2):
            rows = pl.ds(pl.multiple_of(half * 2 * TOK + part * CHUNK, CHUNK), CHUNK)
            pbuf[s, rows, :] += weighted(x2[s, rows, :], g2[rows, :], zc * 8 + s * 4 + slot, slot)

    order = (0, 2, 1, 3)

    def load(zc, slot):
        return lambda: start(w_load(zc, slot))

    def loaded(zc, slot):
        return lambda: wait(w_load(zc, slot))

    plan2 = {
        2: [load(1, 0)],
        4: [lambda: wait_recv(w_forward(0)), load(1, 2)],
        8: [loaded(1, 0), lambda: r2(1), lambda: feed(24)],
        10: [loaded(1, 2)],
        11: [lambda: r45(1)],
    }

    def second_a(m, _):
        hooks(m, plan2)
        i = m // 2
        unit(0, 1 - m % 2, i // 4, (i % 2) * 2 + (i % 4) // 2)
        return 0

    lax.fori_loop(0, 12, second_a, 0)
    pieces_in(1)
    start(w_forward(1))
    load(1, 1)()
    clear(1)
    loaded(1, 1)()

    def arrived():
        wait_recv(w_forward(1))
        start(w_load(1, 3))
        g1(1)
        wait(w_load(1, 3))

    plan3 = {1: [arrived], 2: [lambda: b_far(0)]}

    def second_b(m, _):
        hooks(m, plan3)
        unit(0, 1 - m // 2, 1, 1 + 2 * (m % 2))
        return 0

    lax.fori_loop(0, 4, second_b, 0)
    g_far(1)

    plan4 = {}
    for i in range(4):
        plan4.setdefault(i + 1, []).append(load(0, order[i]))
        plan4.setdefault(i + 9, []).append(load(1, order[i]))
        plan4.setdefault(i + 4, []).append(loaded(0, order[i]))
        plan4.setdefault(i + 12, []).append(loaded(1, order[i]))
    plan4[6].append(lambda: b1(0))
    plan4.setdefault(8, []).append(lambda: b_far(1))

    def second_c(m, _):
        hooks(m, plan4)
        q, j = m // 4, m % 4
        unit(1, 1 - q // 2, 1 - ((q + 1) // 2) % 2, (j % 2) * 2 + j // 2)
        return 0

    lax.fori_loop(0, 16, second_c, 0)
    b2(0)
    b1(1)
    b2(1)
    for s in range(2):
        for cp in [ag(s, k, j) for k in range(N1) for j in range(7)] + [c(s, k, j) for c in (bg, bs) for k in range(N2) for j in range(3)]:
            cp.wait_send()
    for cp in w_second_swap() + w_forward(0) + w_forward(1) + [w_piece(p) for p in range(6 * PIECES)]:
        cp.wait_send()
    for mb in range(2):
        for k in range(2):
            out_store(mb, k).wait()


def solution(mesh):
    tok_spec = P(None, MESH_AXES, None)
    route_spec = P(None, None, MESH_AXES, None)
    weight_spec = P(None, MESH_AXES, None, None)

    def device_body(tokens_in, expert_ids, gate_vals, w_up1, w_up3, w_down):
        any_spec = pl.BlockSpec(memory_space=pl.ANY)
        vmem_spec = pl.BlockSpec(memory_space=pltpu.VMEM)
        dma = pltpu.SemaphoreType.DMA

        def by_slot(route):
            return jnp.swapaxes(route, 2, 3).reshape(-1, route.shape[2])

        return pl.pallas_call(
            moe_kernel,
            name="moe_layers",
            out_shape=[
                jax.ShapeDtypeStruct(tokens_in.shape, BF16),
                jax.ShapeDtypeStruct((6, HID, FFN), BF16),
                jax.ShapeDtypeStruct((6, HID, FFN), BF16),
                jax.ShapeDtypeStruct((6, FFN, HID), BF16),
            ],
            in_specs=[any_spec, vmem_spec, vmem_spec, any_spec, any_spec, any_spec],
            out_specs=[any_spec] * 4,
            scratch_shapes=[
                pltpu.VMEM((2, 8 * TOK, HID), BF16),
                pltpu.VMEM((2, 4 * TOK, HID), BF16),
                pltpu.VMEM((2, 8 * TOK, HID), F32),
                pltpu.VMEM((2, 4 * TOK, HID), F32),
                pltpu.VMEM((2, 2 * TOK, HID), F32),
                pltpu.VMEM((2, TOK, HID), F32),
                pltpu.VMEM((4, HID, FFN), BF16),
                pltpu.VMEM((4, HID, FFN), BF16),
                pltpu.VMEM((4, FFN, HID), BF16),
                pltpu.VMEM((128, TOK), F32),
                pltpu.VMEM((128, TOK), F32),
                pltpu.VMEM((8 * TOK, 128), F32),
                pltpu.VMEM((4 * TOK, 128), F32),
                pltpu.VMEM((2, TOK, HID), BF16),
                dma((2, N1, 7)), dma((2, N1, 7)), dma((2, N1, 5)), dma((2, N1, 5)),
                dma((2, 2, 3)), dma((2, 2, 3)), dma((2, 2, 3)), dma((2, 2, 3)),
                dma((4, 3)), dma((3,)), dma((3,)), dma((3,)), dma((3,)),
                dma((6 * PIECES,)), dma((6 * PIECES,)), dma((2, 3)), dma((2, 3)), dma((10,)), dma((10,)), dma((2, N1)), dma((2, 2)),
            ],
            compiler_params=pltpu.CompilerParams(collective_id=0, has_side_effects=True, vmem_limit_bytes=66 * 10**6),
        )(tokens_in, by_slot(expert_ids), by_slot(gate_vals), w_up1, w_up3, w_down)[0]

    return jax.shard_map(device_body, mesh=mesh, in_specs=(tok_spec, route_spec, route_spec, weight_spec, weight_spec, weight_spec), out_specs=tok_spec, check_vma=False)
```

```python
import jax
import jax.numpy as jnp
from jax import lax
from jax.experimental import pallas as pl
from jax.experimental.pallas import tpu as pltpu
from jax.sharding import PartitionSpec as P

ROUTE_SCALE = 2.5
MESH_AXES = ("ez", "ey", "ex")
MESH = pl.DeviceIdType.MESH
BF16, F32 = jnp.bfloat16, jnp.float32

TOK, HID, FFN = 256, 1024, 512
N1, N2 = 4, 2
ROW1, PART = TOK // N1, TOK // N2
CHUNK = 256
PIECES = 4

AXES1 = (((0, 2, 1), (1, 2, 0)) * 2, ((0, 2, 1), (1, 2, 0), (0, 1, 2), (1, 0, 2)))
AXES2 = ((0, 1), (1, 0))
GATHER1 = ((0, 2, 1), (0, 1, 2), (0, 4, 0), (2, 3, 2), (2, 6, 0), (1, 5, 0), (3, 7, 0))
GATHER2 = ((0, 1, 1), (0, 2, 0), (1, 3, 0))


def base1(place, k):
    return (place // 4) * 4 * TOK + k * 4 * ROW1 + (place % 4) * ROW1


def base2(place, k):
    return (place // 2) * 2 * TOK + k * 2 * PART + (place % 2) * PART


def block_of(place, axes):
    n = len(axes)
    return sum(((place >> (n - 1 - i)) & 1) << axis for i, axis in enumerate(axes))


def moe_kernel(tok, ids, gts, w1h, w3h, w2h, out, f1h, f3h, f2h, xbuf, x2, pbuf, ra, rb, rc, w1, w3, w2, tt, gr, gbuf, g2, fin,
               ag_s, ag_r, rs_s, rs_r, bg_s, bg_r, bs_s, bs_r, wl_s, wr_s, wr_r, wb_s, wb_r, z_s, z_r, fw_s, fw_r, g_s, g_r, t_s, o_s):
    z, y, ex = (lax.axis_index(name) for name in MESH_AXES)
    x, core = ex // 2, ex % 2

    def turned(bu, bv):
        return bu + core * (bv - bu), bv + core * (bu - bv)

    def dev(bu, bv, bz):
        bx, by = turned(bu, bv)
        return (z + bz - 2 * z * bz, y + by - 2 * y * by, (x + bx - 2 * x * bx) * 2 + core)

    nbr = (dev(1, 0, 0), dev(0, 1, 0), dev(0, 0, 1))
    sib = (z, y, x * 2 + 1 - core)

    def remote(src, dst, ss, rs, to):
        return pltpu.make_async_remote_copy(src_ref=src, dst_ref=dst, send_sem=ss, recv_sem=rs, device_id=to, device_id_type=MESH)

    def ag(s, k, j):
        src, dst, which = GATHER1[j]
        return remote(xbuf.at[s, pl.ds(base1(src, k), ROW1)], xbuf.at[s, pl.ds(base1(dst, k), ROW1)],
                      ag_s.at[s, k, j], ag_r.at[s, k, j], nbr[AXES1[s][k][which]])

    def rs(s, k, j):
        if j < 2:
            src, dst, which = pbuf.at[s, pl.ds(base1(6 - 2 * j, k), 2 * ROW1)], ra.at[s, pl.ds((4 * k + 2 - 2 * j) * ROW1, 2 * ROW1)], 0
        elif j < 4:
            src, dst, which = pbuf.at[s, pl.ds(base1(7 - 2 * j, k), ROW1)], rb.at[s, pl.ds((2 * k + 3 - j) * ROW1, ROW1)], 2
        else:
            src, dst, which = pbuf.at[s, pl.ds(base1(2, k), ROW1)], rc.at[s, pl.ds(k * ROW1, ROW1)], 1
        return remote(src, dst, rs_s.at[s, k, j], rs_r.at[s, k, j], nbr[AXES1[s][k][which]])

    def bg(s, k, j):
        src, dst, which = GATHER2[j]
        return remote(x2.at[s, pl.ds(base2(src, k), PART)], x2.at[s, pl.ds(base2(dst, k), PART)],
                      bg_s.at[s, k, j], bg_r.at[s, k, j], nbr[AXES2[k][which]])

    def bs(s, k, j):
        if j < 2:
            src, dst, which = pbuf.at[s, pl.ds(base2(3 - j, k), PART)], ra.at[s, pl.ds((4 * k + 1 - j) * PART, PART)], 0
        else:
            src, dst, which = pbuf.at[s, pl.ds(base2(1, k), PART)], rb.at[s, pl.ds(2 * k * PART, PART)], 1
        return remote(src, dst, bs_s.at[s, k, j], bs_r.at[s, k, j], nbr[AXES2[k][which]])

    def tok_load(mb):
        return [pltpu.make_async_copy(tok.at[mb, pl.ds(k * ROW1, ROW1)], xbuf.at[mb, pl.ds(base1(0, k), ROW1)], t_s.at[mb, k]) for k in range(N1)]

    def out_store(mb, k):
        rows = pl.ds(k * PART, PART)
        return pltpu.make_async_copy(fin.at[mb, rows], out.at[mb, rows], o_s.at[mb, k])

    held = ((w1h, f1h, w1), (w3h, f3h, w3), (w2h, f2h, w2))

    def w_first_local():
        return [pltpu.make_async_copy(h.at[0, e], v.at[e], wl_s.at[e, i]) for e in range(2) for i, (h, _, v) in enumerate(held)]

    def w_first_remote():
        return [remote(h.at[0], v.at[pl.ds(2, 2)], wr_s.at[i], wr_r.at[i], sib) for i, (h, _, v) in enumerate(held)]

    def w_second_swap():
        return [remote(h.at[1], f.at[pl.ds(0, 2)], wb_s.at[i], wb_r.at[i], sib) for i, (h, f, _) in enumerate(held)]

    def w_piece(p):
        e, i, q = p // (3 * PIECES), (p // PIECES) % 3, p % PIECES
        h, f, _ = held[i]
        rows = pl.ds(q * (h.shape[2] // PIECES), h.shape[2] // PIECES)
        return remote(h.at[1, e, rows], f.at[2 + e, rows], z_s.at[p], z_r.at[p], nbr[2])

    def w_forward(e):
        return [remote(f.at[2 + e], f.at[4 + e], fw_s.at[e, i], fw_r.at[e, i], sib) for i, (_, f, _) in enumerate(held)]

    def w_load(zc, slot):
        if zc:
            srcs = [f.at[2 + slot] for _, f, _ in held]
        else:
            srcs = [h.at[1, slot] if slot < 2 else f.at[slot - 2] for h, f, _ in held]
        return [pltpu.make_async_copy(src, held[i][2].at[slot], wl_s.at[slot, i]) for i, src in enumerate(srcs)]

    def start(copies):
        for cp in copies:
            cp.start()

    def wait(copies):
        for cp in copies:
            cp.wait()

    def wait_recv(copies):
        for cp in copies:
            cp.wait_recv()

    def pieces_in(e):
        wait_recv([w_piece(p) for p in range(e * 3 * PIECES, (e + 1) * 3 * PIECES)])

    fed = [0]

    def feed(n):
        while n and fed[0] < 6 * PIECES:
            w_piece(fed[0]).start()
            fed[0] += 1
            n -= 1

    gate_rows = [(16 * r, 16, r) for r in (1, 2, 3)] + [(16 * (r + 4) + 8, 8, r) for r in (1, 2, 3)] + [(16 * r, 8, r) for r in (4, 5, 6, 7)]

    def gate_copies():
        return [remote(tt.at[pl.ds(row, n)], gr.at[pl.ds(row, n)], g_s.at[i], g_r.at[i], dev(r & 1, (r >> 1) & 1, r >> 2))
                for i, (row, n, r) in enumerate(gate_rows)]

    def ag_begin(s, *js):
        for j in js:
            for k in range(N1):
                ag(s, k, j).start()

    def f1(s):
        for k in range(N1):
            ag(s, k, 0).wait_recv()
            ag(s, k, 3).start()
            ag(s, k, 4).start()

    def f2(s):
        for k in range(N1):
            ag(s, k, 1).wait_recv()
            ag(s, k, 5).start()

    def f3(s, k):
        ag(s, k, 3).wait_recv()
        ag(s, k, 6).start()

    def far(s, k):
        for j in (2, 4, 5, 6):
            ag(s, k, j).wait_recv()

    def add(s, row, n, src):
        rows = pl.ds(row, n)
        pbuf[s, rows] = pbuf[s, rows] + src

    def r1(s):
        for k in range(N1):
            rs(s, k, 0).wait_recv()
            add(s, base1(2, k), 2 * ROW1, ra[s, pl.ds((4 * k + 2) * ROW1, 2 * ROW1)])
            rs(s, k, 2).start()

    def r2(s, ks=range(N1)):
        for k in ks:
            rs(s, k, 1).wait_recv()
            add(s, base1(0, k), 2 * ROW1, ra[s, pl.ds(4 * k * ROW1, 2 * ROW1)])
            rs(s, k, 3).start()

    def r3(s):
        for k in range(N1):
            rs(s, k, 2).wait_recv()
            add(s, base1(2, k), ROW1, rb[s, pl.ds((2 * k + 1) * ROW1, ROW1)])
            rs(s, k, 4).start()

    def r45(s, ks=range(N1)):
        for k in ks:
            rs(s, k, 3).wait_recv()
            rs(s, k, 4).wait_recv()
            rows = pl.ds(base1(0, k), ROW1)
            total = pbuf[s, rows] + rb[s, pl.ds(2 * k * ROW1, ROW1)] + rc[s, pl.ds(k * ROW1, ROW1)]
            into = base2(0, k * N2 // N1) + (k * ROW1) % PART
            x2[s, pl.ds(into, ROW1)] = (xbuf[s, rows].astype(F32) + ROUTE_SCALE * total).astype(BF16)
            if (k + 1) * ROW1 % PART == 0:
                bg(s, k * N2 // N1, 0).start()
                bg(s, k * N2 // N1, 1).start()

    def clear(s):
        for k in range(N1):
            for j in range(5):
                rs(s, k, j).wait_send()
        pbuf[s, pl.ds(0, 4 * TOK)] = jnp.zeros((4 * TOK, HID), F32)

    def g1(s):
        for k in range(2):
            bg(s, k, 0).wait_recv()
            bg(s, k, 2).start()

    def g_far(s):
        for k in range(2):
            bg(s, k, 1).wait_recv()
            bg(s, k, 2).wait_recv()

    def b_far(s):
        for j in range(2):
            for k in range(2):
                bs(s, k, j).start()

    def b1(s):
        for k in range(2):
            bs(s, k, 0).wait_recv()
            add(s, base2(1, k), PART, ra[s, pl.ds((4 * k + 1) * PART, PART)])
            bs(s, k, 2).start()

    def b2(s):
        for k in range(2):
            bs(s, k, 1).wait_recv()
            bs(s, k, 2).wait_recv()
            rows = pl.ds(base2(0, k), PART)
            total = pbuf[s, rows] + ra[s, pl.ds(4 * k * PART, PART)] + rb[s, pl.ds(2 * k * PART, PART)]
            fin[s, pl.ds(k * PART, PART)] = (x2[s, rows].astype(F32) + ROUTE_SCALE * total).astype(BF16)
            out_store(s, k).start()

    start(tok_load(0) + tok_load(1))
    start(w_first_local())
    barrier = pltpu.get_barrier_semaphore()
    for r in range(1, 8):
        pl.semaphore_signal(barrier, inc=1, device_id=dev(r & 1, (r >> 1) & 1, (r >> 2) & 1), device_id_type=MESH)
    pl.semaphore_signal(barrier, inc=1, device_id=sib, device_id_type=MESH)
    pl.semaphore_wait(barrier, 8)
    wait(tok_load(0))
    ag_begin(0, 0, 2, 1)
    wait(tok_load(1))
    ag_begin(1, 0)
    start(w_first_remote())

    row = lax.broadcasted_iota(jnp.int32, (128, TOK), 0)
    rel = row // 16
    bx, by = turned(rel % 2, (rel // 2) % 2)
    bz = rel // 4
    chip = (x + bx - 2 * x * bx) + 2 * (y + by - 2 * y * by) + 4 * (z + bz - 2 * z * bz)
    expert = 4 * chip + (row % 4 + 2 * core) % 4
    table = jnp.zeros((128, TOK), F32)
    for s in range(4):
        wanted = jnp.where((row % 16) // 4 == s, expert, -1)
        for j in range(8):
            i = 8 * s + j
            table = jnp.where(wanted == ids[i:i + 1, :], gts[i:i + 1, :], table)
    tt[...] = table
    start(gate_copies())
    gr[pl.ds(0, 16)] = tt[pl.ds(0, 16)]
    gr[pl.ds(72, 8)] = tt[pl.ds(72, 8)]

    f1(0)
    f2(0)
    feed(2)
    wait(gate_copies())
    by_token = gr[...].T

    def lanes(piece, first, second, cut):
        spot = lax.broadcasted_iota(jnp.int32, piece.shape, 1)
        return jnp.where(spot < cut, pltpu.roll(piece, (128 - first) % 128, axis=1), pltpu.roll(piece, (cut + 128 - second) % 128, axis=1))

    for k in range(N1):
        for place in range(8):
            r_0, r_1 = block_of(place, AXES1[0][k]), block_of(place, AXES1[1][k])
            gbuf[pl.ds(base1(place, k), ROW1), :] = lanes(by_token[k * ROW1:(k + 1) * ROW1, :], 16 * r_0, 16 * r_1 + 4, 4)
    for k in range(N2):
        for place in range(4):
            r = block_of(place, AXES2[k])
            g2[pl.ds(base2(place, k), PART), :] = lanes(by_token[k * PART:(k + 1) * PART, :], 16 * r + 8, 16 * (r + 4) + 8, 8)
    wait(w_first_local() + w_first_remote())

    lane = lax.broadcasted_iota(jnp.int32, (CHUNK, 128), 1)

    def weighted(x_blk, g_blk, column, slot):
        a = jnp.dot(x_blk, w1[slot], preferred_element_type=F32)
        b = jnp.dot(x_blk, w3[slot], preferred_element_type=F32)
        h = (jax.nn.silu(a) * b).astype(BF16)
        o = jnp.dot(h, w2[slot], preferred_element_type=F32).astype(BF16).astype(F32)
        g = jnp.sum(jnp.where(lane == column, g_blk, 0.0), axis=1, keepdims=True)
        return jnp.where(g > 0.0, g * o, 0.0)

    def hooks(n, plan):
        for when in sorted(plan):
            @pl.when(n == when)
            def _():
                for step in plan[when]:
                    step()

    def send(k):
        return lambda: start([rs(0, k, 0), rs(0, k, 1)])

    plan1 = {n: [lambda: feed(1)] for n in range(16)}
    plan1[0] += [lambda: f3(0, 0)]
    plan1[1] += [lambda: f3(0, 1), lambda: f3(0, 2), lambda: f3(0, 3), lambda: ag_begin(1, 2, 1), lambda: f1(1)]
    plan1[4] += [lambda: far(0, 0)]
    plan1[5] += [lambda: far(0, 1), lambda: f2(1)]
    plan1[6] += [lambda: far(0, 2)] + [lambda k=k: f3(1, k) for k in range(N1)] + [send(0), send(1)]
    plan1[7] += [lambda: far(0, 3), send(2)]
    plan1[8] += [send(3)]
    plan1[9] += [lambda: start(w_second_swap())]
    for k in range(N1):
        plan1[12 + k] += [lambda k=k: far(1, k)]

    def layer1(n, _):
        hooks(n, plan1)
        s = n // 8
        rows = pl.ds(pl.multiple_of((n % 8) * CHUNK, CHUNK), CHUNK)
        x_blk, g_blk = xbuf[s, rows, :], gbuf[rows, :]
        for e in range(4):
            term = weighted(x_blk, g_blk, s * 4 + e, e)
            pbuf[s, rows, :] = term if e == 0 else pbuf[s, rows, :] + term
        return 0

    lax.fori_loop(0, 16, layer1, 0)

    start(w_load(0, 0) + w_load(0, 1))
    r1(0)
    wait_recv(w_second_swap())
    start(w_load(0, 2) + w_load(0, 3))
    pieces_in(0)
    start(w_forward(0))
    r2(0)
    start([rs(1, k, 0) for k in range(N1)])
    r3(0)
    feed(1)
    r45(0)
    r1(1)
    feed(2)
    g1(0)
    start([rs(1, k, 1) for k in (2, 3, 0, 1)])
    clear(0)
    r3(1)
    feed(2)
    for slot in range(4):
        wait(w_load(0, slot))
    g_far(0)

    def unit(s, half, zc, slot):
        for part in range(2):
            rows = pl.ds(pl.multiple_of(half * 2 * TOK + part * CHUNK, CHUNK), CHUNK)
            pbuf[s, rows, :] += weighted(x2[s, rows, :], g2[rows, :], zc * 8 + s * 4 + slot, slot)

    order = (0, 2, 1, 3)

    def load(zc, slot):
        return lambda: start(w_load(zc, slot))

    def loaded(zc, slot):
        return lambda: wait(w_load(zc, slot))

    plan2 = {
        2: [load(1, 0)],
        4: [lambda: wait_recv(w_forward(0)), load(1, 2), lambda: r2(1, (2, 3))],
        8: [loaded(1, 0), lambda: r2(1, (0, 1)), lambda: feed(24)],
        10: [loaded(1, 2)],
        11: [lambda: r45(1, (2, 3, 0, 1))],
    }

    def second_a(m, _):
        hooks(m, plan2)
        i = m // 2
        unit(0, 1 - m % 2, i // 4, (i % 2) * 2 + (i % 4) // 2)
        return 0

    lax.fori_loop(0, 12, second_a, 0)
    pieces_in(1)
    start(w_forward(1))
    load(1, 1)()
    clear(1)
    loaded(1, 1)()

    def arrived():
        wait_recv(w_forward(1))
        start(w_load(1, 3))
        g1(1)
        wait(w_load(1, 3))

    plan3 = {1: [arrived], 2: [lambda: b_far(0)]}

    def second_b(m, _):
        hooks(m, plan3)
        unit(0, 1 - m // 2, 1, 1 + 2 * (m % 2))
        return 0

    lax.fori_loop(0, 4, second_b, 0)
    g_far(1)

    plan4 = {}
    for i in range(4):
        plan4.setdefault(i + 1, []).append(load(0, order[i]))
        plan4.setdefault(i + 9, []).append(load(1, order[i]))
        plan4.setdefault(i + 4, []).append(loaded(0, order[i]))
        plan4.setdefault(i + 12, []).append(loaded(1, order[i]))
    plan4[6].append(lambda: b1(0))
    plan4.setdefault(8, []).append(lambda: b_far(1))

    def second_c(m, _):
        hooks(m, plan4)
        q, j = m // 4, m % 4
        unit(1, 1 - q // 2, 1 - ((q + 1) // 2) % 2, (j % 2) * 2 + j // 2)
        return 0

    lax.fori_loop(0, 16, second_c, 0)
    b2(0)
    b1(1)
    b2(1)
    for s in range(2):
        for cp in [ag(s, k, j) for k in range(N1) for j in range(7)] + [c(s, k, j) for c in (bg, bs) for k in range(N2) for j in range(3)]:
            cp.wait_send()
    for cp in w_second_swap() + w_forward(0) + w_forward(1) + [w_piece(p) for p in range(6 * PIECES)]:
        cp.wait_send()
    for mb in range(2):
        for k in range(2):
            out_store(mb, k).wait()


def solution(mesh):
    tok_spec = P(None, MESH_AXES, None)
    route_spec = P(None, None, MESH_AXES, None)
    weight_spec = P(None, MESH_AXES, None, None)

    def device_body(tokens_in, expert_ids, gate_vals, w_up1, w_up3, w_down):
        any_spec = pl.BlockSpec(memory_space=pl.ANY)
        vmem_spec = pl.BlockSpec(memory_space=pltpu.VMEM)
        dma = pltpu.SemaphoreType.DMA

        def by_slot(route):
            return jnp.swapaxes(route, 2, 3).reshape(-1, route.shape[2])

        return pl.pallas_call(
            moe_kernel,
            name="moe_layers",
            out_shape=[
                jax.ShapeDtypeStruct(tokens_in.shape, BF16),
                jax.ShapeDtypeStruct((6, HID, FFN), BF16),
                jax.ShapeDtypeStruct((6, HID, FFN), BF16),
                jax.ShapeDtypeStruct((6, FFN, HID), BF16),
            ],
            in_specs=[any_spec, vmem_spec, vmem_spec, any_spec, any_spec, any_spec],
            out_specs=[any_spec] * 4,
            scratch_shapes=[
                pltpu.VMEM((2, 8 * TOK, HID), BF16),
                pltpu.VMEM((2, 4 * TOK, HID), BF16),
                pltpu.VMEM((2, 8 * TOK, HID), F32),
                pltpu.VMEM((2, 4 * TOK, HID), F32),
                pltpu.VMEM((2, 2 * TOK, HID), F32),
                pltpu.VMEM((2, TOK, HID), F32),
                pltpu.VMEM((4, HID, FFN), BF16),
                pltpu.VMEM((4, HID, FFN), BF16),
                pltpu.VMEM((4, FFN, HID), BF16),
                pltpu.VMEM((128, TOK), F32),
                pltpu.VMEM((128, TOK), F32),
                pltpu.VMEM((8 * TOK, 128), F32),
                pltpu.VMEM((4 * TOK, 128), F32),
                pltpu.VMEM((2, TOK, HID), BF16),
                dma((2, N1, 7)), dma((2, N1, 7)), dma((2, N1, 5)), dma((2, N1, 5)),
                dma((2, 2, 3)), dma((2, 2, 3)), dma((2, 2, 3)), dma((2, 2, 3)),
                dma((4, 3)), dma((3,)), dma((3,)), dma((3,)), dma((3,)),
                dma((6 * PIECES,)), dma((6 * PIECES,)), dma((2, 3)), dma((2, 3)), dma((10,)), dma((10,)), dma((2, N1)), dma((2, 2)),
            ],
            compiler_params=pltpu.CompilerParams(collective_id=0, has_side_effects=True, vmem_limit_bytes=66 * 10**6),
        )(tokens_in, by_slot(expert_ids), by_slot(gate_vals), w_up1, w_up3, w_down)[0]

    return jax.shard_map(device_body, mesh=mesh, in_specs=(tok_spec, route_spec, route_spec, weight_spec, weight_spec, weight_spec), out_specs=tok_spec, check_vma=False)
```
